256 devices in a mesh: depth: 2 (over z_hi), row: 8 (over y, core), col: 16 (over x, z_lo).
Axes of the slice: x: 4, y: 4, z: 8 (z_hi: 2, z_lo: 4; z = z_hi * 4 + z_lo), core: 2. Of those that a mesh axis runs over, the one named last changes fastest.
Arguments:
- q_slab: float32 [6144, 1024], P('col', ('depth', 'row')), may hold values from -6 to 6
- triangle: float32 [1024, 1024], P(None, 'depth'), as said below
- panel_q: float32 [32768, 1024], P('row', ('depth', 'col')), may hold values from -0.1875 to 0.1875
Outputs:
- slab_out: float32 [6144, 32768], P('col', 'row')
The draws below stay inside these ranges and needn't reach their ends.
Inputs may be any that keep to these rules, and one draw needn't show every extreme that they name: triangle is zero below its diagonal; its diagonal lies in 0.5 to 1.5.
All inputs are finite; a program needn't handle non-finite values.
Results may differ from the reference program's by a relative error of at most 0.000071.
Values sent between devices are 32-bit elements; how exact they have to be, the bound alone decides.
A program may use at most 64 MiB of HBM per device.

```python
import math
import jax
import jax.numpy as jnp
from jax import lax

ORDER = 32768
K = 1024
SLAB = 6144


def draw_triangle(key, part):
    first, second = jax.random.split(jax.random.fold_in(key, 7))
    upper = jnp.clip(jax.random.normal(first, (K, K), jnp.float32), -4.0, 4.0)
    upper = upper / math.sqrt(K)
    diagonal = jax.random.uniform(second, (K,), jnp.float32, 0.5, 1.5)
    return jnp.triu(upper, 1) + jnp.diag(diagonal)


def block_levels(rng, shape, shards, low, largest):
    def one(dim, shards_of):
        heights = jax.random.uniform(jax.random.fold_in(jax.random.fold_in(rng, 6), dim), (shards_of,), jnp.float32, low / len(shards), largest / len(shards))
        return jnp.repeat(jnp.exp(heights), shape[dim] // shards_of).reshape((-1,) + (1,) * (len(shape) - dim - 1))

    gain = one(*shards[0])
    for cut in shards[1:]:
        gain = gain * one(*cut)
    return gain


def gaussian(key, shape, deviation, most, cuts=(), dtype=jnp.bfloat16):
    array = deviation * jax.random.normal(key, shape, jnp.float32)
    if cuts:
        array = array * block_levels(key, shape, cuts, -0.22, 0.18)
    return jnp.clip(array, -most, most).astype(dtype)


def setup_inputs(seed: int = 0) -> dict:
    seeds = jax.random.split(jax.random.key(seed), 4)
    q_slab = gaussian(seeds[0], (SLAB, K), 1.0, 6.0, ((0, 16), (1, 16)), jnp.float32)
    triangle = draw_triangle(jax.random.fold_in(seeds[3], 71), 0)
    panel_q = gaussian(seeds[2], (ORDER, K), K ** -0.5, 0.1875, ((0, 8), (1, 32)), jnp.float32)
    return {"q_slab": q_slab, "triangle": triangle, "panel_q": panel_q}


def reference(q_slab, triangle, panel_q):
    left = jnp.dot(q_slab, triangle, precision=lax.Precision.HIGHEST, preferred_element_type=jnp.float32)
    return lax.dot_general(left, panel_q, (((1,), (1,)), ((), ())), precision=lax.Precision.HIGHEST, preferred_element_type=jnp.float32)
```

```python
import functools

import jax
import jax.numpy as jnp
from jax import lax
from jax.experimental import pallas as pl
from jax.experimental.pallas import tpu as pltpu
from jax.sharding import Mesh
from jax.sharding import PartitionSpec as P

AXES = ("depth", "y", "core", "x", "zl")
MESH = pl.DeviceIdType.MESH
F32, BF16 = jnp.float32, jnp.bfloat16


def split(value):
    high = value.astype(BF16)
    return high, (value - high.astype(F32)).astype(BF16)


def dot(a, b):
    return jnp.dot(a, b, preferred_element_type=F32)


def kernel(dims, unit, q_ref, t_ref, p_ref, out_ref,
           qbuf, qrow, lf, lhi, llo, gat, phi, plo, obuf,
           q_send, q_recv, e_send, e_recv, e_own, z_send, z_recv,
           d_send, d_recv, lx_send, lx_recv, y_send, y_recv,
           c_send, c_recv, o_own, o_send, o_recv):
    nd, ny, nc, nx, nzl = dims
    nz = nd * nzl
    nr = ny * nc
    nb = nd * nr
    d, y, core, x, zl = (lax.axis_index(a) for a in AXES)
    z = d * nzl + zl
    rk = y * nc + core
    me_b = d * nr + rk
    chunks = gat.shape[0]
    piece = lf.shape[3]
    half = lf.shape[4]
    k_full = nd * half
    rows = nr * piece
    qk = q_ref.shape[1]

    def dev(**over):
        return tuple(over.get(a, v) for a, v in zip(AXES, (d, y, core, x, zl)))

    def at_z(pos):
        pos = lax.rem(pos + nz, nz)
        return lax.div(pos, nzl), lax.rem(pos, nzl)

    def at_b(pos):
        pos = lax.rem(pos, nb)
        dd, r = lax.div(pos, nr), lax.rem(pos, nr)
        return dd, lax.div(r, nc), lax.rem(r, nc), r

    def remote(src, dst, send, recv, to):
        return pltpu.make_async_remote_copy(
            src_ref=src, dst_ref=dst, send_sem=send, recv_sem=recv,
            device_id=to, device_id_type=MESH)

    def role_of(pos, j):
        return lax.rem(pos + j, 2)

    barrier = pltpu.get_barrier_semaphore()
    for o in range(1, nb):
        dd, yy, cc, _ = at_b(me_b + o)
        pl.semaphore_signal(barrier, inc=1, device_id=dev(depth=dd, y=yy, core=cc), device_id_type=MESH)
    for o in range(1, nx):
        pl.semaphore_signal(barrier, inc=1, device_id=dev(x=lax.rem(x + o, nx)), device_id_type=MESH)
    for o in (1, nz - 1):
        dd, zz = at_z(z + o)
        pl.semaphore_signal(barrier, inc=1, device_id=dev(depth=dd, zl=zz), device_id_type=MESH)
    pl.semaphore_wait(barrier, nb - 1 + nx - 1 + 2)

    def q_copy(o):
        dd, yy, cc, r = at_b(me_b + o)
        src = q_ref.at[pl.ds(pl.multiple_of(r * piece, 8), piece)]
        return remote(src, qbuf.at[me_b], q_send.at[o], q_recv.at[o], dev(depth=dd, y=yy, core=cc))

    def q_arrival(o):
        src = lax.rem(me_b + nb - o, nb)
        dd, yy, cc, _ = at_b(src)
        return remote(qbuf.at[src], qbuf.at[src], q_send.at[o], q_recv.at[o], dev(depth=dd, y=yy, core=cc))

    def q_start(o, _):
        q_copy(o).start()
        return 0

    lax.fori_loop(1, nb, q_start, 0)

    def e_copy(j, o):
        to = lax.rem(x + o, nx)
        block = 2 * j + role_of(to, j)
        src = p_ref.at[:, pl.ds(pl.multiple_of(block * unit, unit), unit)]
        return remote(src, gat.at[j, d, x, zl], e_send.at[j, o], e_recv.at[j, o], dev(x=to))

    def e_arrival(j, o):
        src = lax.rem(x + nx - o, nx)
        ref = gat.at[j, d, src, zl]
        return remote(ref, ref, e_send.at[j, o], e_recv.at[j, o], dev(x=src))

    def e_local(j):
        block = 2 * j + role_of(x, j)
        src = p_ref.at[:, pl.ds(pl.multiple_of(block * unit, unit), unit)]
        return pltpu.make_async_copy(src, gat.at[j, d, x, zl], e_own.at[j])

    def e_start(j, _):
        e_local(j).start()
        for o in range(1, nx):
            e_copy(j, o).start()
        return 0

    lax.fori_loop(0, chunks, e_start, 0)

    nlong, nshort = nz // 2, (nz - 1) // 2

    def z_copy(j, hop, far):
        sign = 1 - 2 * lax.rem(j, 2)
        step = sign if far else -sign
        index = hop - 1 if far else nlong + hop - 1
        dd, zz = at_z(z - step * (hop - 1))
        to_d, to_z = at_z(z + step)
        ref = gat.at[j, dd, :, zz]
        return remote(ref, ref, z_send.at[j, index], z_recv.at[j, index], dev(depth=to_d, zl=to_z))

    def z_arrival(j, hop, far):
        sign = 1 - 2 * lax.rem(j, 2)
        step = sign if far else -sign
        index = hop - 1 if far else nlong + hop - 1
        dd, zz = at_z(z - step * hop)
        from_d, from_z = at_z(z - step)
        ref = gat.at[j, dd, :, zz]
        return remote(ref, ref, z_send.at[j, index], z_recv.at[j, index], dev(depth=from_d, zl=from_z))

    def hop(j, h):
        if h == 1:
            e_local(j).wait()
            for o in range(1, nx):
                e_arrival(j, o).wait_recv()
        for far, count in ((True, nlong), (False, nshort)):
            if 2 <= h <= count + 1:
                z_arrival(j, h - 1, far).wait_recv()
            if h <= count:
                z_copy(j, h, far).start()

    def left_piece():
        qbuf[me_b] = q_ref[pl.ds(pl.multiple_of(rk * piece, 8), piece), :]

        def q_wait(o, _):
            q_arrival(o).wait_recv()
            return 0

        lax.fori_loop(1, nb, q_wait, 0)
        for b in range(nb):
            qrow[:, b * qk:(b + 1) * qk] = qbuf[b]
        qh, ql = split(qrow[...])
        th, tl = split(t_ref[...])
        lf[d, x, rk] = dot(qh, th) + dot(qh, tl) + dot(ql, th)

    def depth_copy(dd):
        ref = lf.at[dd, x, rk]
        return remote(ref, ref, d_send.at[0], d_recv.at[0], dev(depth=1 - d))

    def lx_copy(o):
        ref = lf.at[:, x, rk]
        return remote(ref, ref, lx_send.at[o], lx_recv.at[o], dev(x=lax.rem(x + o, nx)))

    def lx_arrival(o):
        src = lax.rem(x + nx - o, nx)
        ref = lf.at[:, src, rk]
        return remote(ref, ref, lx_send.at[o], lx_recv.at[o], dev(x=src))

    ylong, yshort = ny // 2, (ny - 1) // 2

    def y_index(h, far):
        return h - 1 if far else ylong + h - 1

    def y_step(xs, far):
        sign = 1 - 2 * lax.rem(xs, 2)
        return sign if far else -sign

    def y_copy(xs, h, far):
        step = y_step(xs, far)
        owner = lax.rem(y - step * (h - 1) + ny, ny)
        ref = lf.at[:, xs, owner * nc + core]
        i = y_index(h, far)
        return remote(ref, ref, y_send.at[xs, i], y_recv.at[xs, i], dev(y=lax.rem(y + step + ny, ny)))

    def y_arrival(xs, h, far):
        step = y_step(xs, far)
        owner = lax.rem(y - step * h + ny, ny)
        ref = lf.at[:, xs, owner * nc + core]
        i = y_index(h, far)
        return remote(ref, ref, y_send.at[xs, i], y_recv.at[xs, i], dev(y=lax.rem(y - step + ny, ny)))

    def c_copy(xs, h, far, arriving=False):
        owner = lax.rem(y - y_step(xs, far) * h + ny, ny)
        i = 0 if h == 0 else 1 + y_index(h, far)
        ref = lf.at[:, xs, owner * nc + (1 - core if arriving else core)]
        return remote(ref, ref, c_send.at[xs, i], c_recv.at[xs, i], dev(core=1 - core))

    def y_first(xs):
        c_copy(xs, 0, True).start()
        for far, count in ((True, ylong), (False, yshort)):
            if count >= 1:
                y_copy(xs, 1, far).start()

    def y_later(xs, h):
        for far, count in ((True, ylong), (False, yshort)):
            if 1 <= h - 1 <= count:
                y_arrival(xs, h - 1, far).wait_recv()
                if h <= count:
                    y_copy(xs, h, far).start()
                c_copy(xs, h - 1, far).start()

    def y_blocks():
        return [(0, True)] + [(h, True) for h in range(1, ylong + 1)] + [(h, False) for h in range(1, yshort + 1)]

    def each_xs(body):
        def step(o, _):
            body(lax.rem(x + o, nx))
            return 0
        lax.fori_loop(0, nx, step, 0)

    def left_ready(xs):
        for h, far in y_blocks():
            c_copy(xs, h, far, arriving=True).wait_recv()
        for b in range(nd):
            high, low = split(lf[b, xs].reshape(rows, half))
            lhi[xs, :, b * half:(b + 1) * half] = high
            llo[xs, :, b * half:(b + 1) * half] = low

    def partner_of(j):
        return lax.rem(x + 1 - 2 * role_of(x, j) + nx, nx)

    def own_copy(j):
        block = 2 * j + role_of(x, j)
        dst = out_ref.at[:, pl.ds(pl.multiple_of(block * unit, unit), unit)]
        return pltpu.make_async_copy(obuf.at[j, 0], dst, o_own.at[j])

    def ship_copy(j, arriving=False):
        block = 2 * j + (1 - role_of(x, j) if arriving else role_of(x, j))
        dst = out_ref.at[:, pl.ds(pl.multiple_of(block * unit, unit), unit)]
        return remote(obuf.at[j, 1], dst, o_send.at[j], o_recv.at[j], dev(x=partner_of(j)))

    def compute(j):
        if nlong > 3:
            z_arrival(j, nlong, True).wait_recv()
        high, low = split(gat[j].reshape(k_full, unit))
        phi[...] = high
        plo[...] = low

        def product(xs):
            return (dot(lhi[xs], phi[...]) + dot(lhi[xs], plo[...])) + dot(llo[xs], phi[...])

        def side(s, _):
            xs = jnp.where(s == 0, partner_of(j), x)
            obuf[j, 1 - s] = product(xs)
            return 0

        obuf[j, 1] = product(partner_of(j))
        ship_copy(j).start()
        obuf[j, 0] = product(x)
        own_copy(j).start()

    hop(0, 1)
    left_piece()
    depth_copy(d).start()
    hop(0, 2)
    hop(1, 1)
    depth_copy(1 - d).wait_recv()
    for o in range(1, nx):
        lx_copy(o).start()
    y_first(x)
    hop(0, 3)
    hop(1, 2)
    for o in range(1, nx):
        lx_arrival(o).wait_recv()
        y_first(lax.rem(x + nx - o, nx))
    hop(0, 4)
    hop(1, 3)
    hop(2, 1)
    for h in range(2, ylong + 1):
        each_xs(functools.partial(y_later, h=h))
    hop(1, 4)
    hop(2, 2)
    each_xs(functools.partial(y_later, h=ylong + 1))
    each_xs(left_ready)

    def body(i, _):
        @pl.when(i - 1 < chunks)
        def _():
            hop(i - 1, 3)

        @pl.when(i < chunks)
        def _():
            hop(i, 1)

        compute(i - 3)

        @pl.when(i - 1 < chunks)
        def _():
            hop(i - 1, 4)

        @pl.when(i < chunks)
        def _():
            hop(i, 2)

        return 0

    lax.fori_loop(3, chunks + 3, body, 0)

    def finish(j, _):
        own_copy(j).wait()
        ship_copy(j).wait_send()
        ship_copy(j, arriving=True).wait_recv()
        for o in range(1, nx):
            e_copy(j, o).wait_send()
        for h in range(1, nlong + 1):
            z_copy(j, h, True).wait_send()
        for h in range(1, nshort + 1):
            z_copy(j, h, False).wait_send()
        return 0

    lax.fori_loop(0, chunks, finish, 0)

    def q_finish(o, _):
        q_copy(o).wait_send()
        return 0

    lax.fori_loop(1, nb, q_finish, 0)
    depth_copy(d).wait_send()
    for o in range(1, nx):
        lx_copy(o).wait_send()

    def y_finish(xs):
        for h, far in y_blocks():
            c_copy(xs, h, far).wait_send()
            if h:
                y_copy(xs, h, far).wait_send()

    each_xs(y_finish)


def per_device(dims, unit, q_slab, triangle, panel_q):
    nd, ny, nc, nx, nzl = dims
    nz, nr, nb = nd * nzl, ny * nc, nd * ny * nc
    rows, qk = q_slab.shape
    k_full, half = triangle.shape
    out_cols, narrow = panel_q.shape
    chunks = out_cols // (2 * unit)
    dma = pltpu.SemaphoreType.DMA
    vmem = pl.BlockSpec(memory_space=pltpu.VMEM)
    return pl.pallas_call(
        functools.partial(kernel, dims, unit),
        out_shape=jax.ShapeDtypeStruct((rows, out_cols), F32),
        in_specs=[vmem] * 3,
        out_specs=pl.BlockSpec(memory_space=pl.ANY),
        scratch_shapes=[
            pltpu.VMEM((nb, rows // nr, qk), F32),
            pltpu.VMEM((rows // nr, k_full), F32),
            pltpu.VMEM((nd, nx, nr, rows // nr, half), F32),
            pltpu.VMEM((nx, rows, k_full), BF16),
            pltpu.VMEM((nx, rows, k_full), BF16),
            pltpu.VMEM((chunks, nd, nx, nzl, narrow, unit), F32),
            pltpu.VMEM((k_full, unit), BF16),
            pltpu.VMEM((k_full, unit), BF16),
            pltpu.VMEM((chunks, 2, rows, unit), F32),
            dma((nb,)), dma((nb,)),
            dma((chunks, nx)), dma((chunks, nx)), dma((chunks,)),
            dma((chunks, nz)), dma((chunks, nz)),
            dma((1,)), dma((1,)),
            dma((nx,)), dma((nx,)),
            dma((nx, ny)), dma((nx, ny)),
            dma((nx, ny)), dma((nx, ny)),
            dma((chunks,)), dma((chunks,)), dma((chunks,)),
        ],
        compiler_params=pltpu.CompilerParams(
            collective_id=0, has_side_effects=True, vmem_limit_bytes=60 * 1024 * 1024
        ),
    )(q_slab, triangle, panel_q.T)


def build(mesh, dims, unit):
    torus = Mesh(mesh.devices.reshape(dims), AXES)
    slab = ("x", "zl")
    row = ("y", "core")
    in_specs = (P(slab, ("depth",) + row), P(None, "depth"), P(row, ("depth",) + slab))
    return jax.shard_map(
        functools.partial(per_device, dims, unit),
        mesh=torus, in_specs=in_specs, out_specs=P(slab, row), check_vma=False)


def solution(mesh):
    return build(mesh, (mesh.shape["depth"], 4, 2, 4, 4), 256)
```

```python
import functools

import jax
import jax.numpy as jnp
from jax import lax
from jax.experimental import pallas as pl
from jax.experimental.pallas import tpu as pltpu
from jax.sharding import Mesh
from jax.sharding import PartitionSpec as P

AXES = ("depth", "y", "core", "x", "zl")
MESH = pl.DeviceIdType.MESH
F32, BF16 = jnp.float32, jnp.bfloat16


def split(value):
    high = value.astype(BF16)
    return high, (value - high.astype(F32)).astype(BF16)


def dot(a, b):
    return jnp.dot(a, b, preferred_element_type=F32)


def kernel(dims, unit, groups, q_ref, t_hbm, p_hbm, out_ref,
           qs, t_ref, p_ref, qbuf, qrow, lf, lhi, llo, gat, phi, plo, obuf, in_sem,
           q_send, q_recv, e_send, e_recv, e_own, z_send, z_recv,
           d_send, d_recv, lx_send, lx_recv, y_send, y_recv,
           c_send, c_recv, o_own, o_send, o_recv):
    wide, pairs = groups
    nd, ny, nc, nx, nzl = dims
    nz = nd * nzl
    nr = ny * nc
    nb = nd * nr
    d, y, core, x, zl = (lax.axis_index(a) for a in AXES)
    z = d * nzl + zl
    rk = y * nc + core
    me_b = d * nr + rk
    chunks = 2 * pairs
    ahead = 6
    piece = lf.shape[3]
    half = lf.shape[4]
    k_full = nd * half
    rows = nr * piece
    qk = qs.shape[1]

    def dev(**over):
        return tuple(over.get(a, v) for a, v in zip(AXES, (d, y, core, x, zl)))

    def at_z(pos):
        pos = lax.rem(pos + nz, nz)
        return lax.div(pos, nzl), lax.rem(pos, nzl)

    def at_b(pos):
        pos = lax.rem(pos, nb)
        dd, r = lax.div(pos, nr), lax.rem(pos, nr)
        return dd, lax.div(r, nc), lax.rem(r, nc), r

    def remote(src, dst, send, recv, to):
        return pltpu.make_async_remote_copy(
            src_ref=src, dst_ref=dst, send_sem=send, recv_sem=recv,
            device_id=to, device_id_type=MESH)

    def base(m):
        return 2 * m + 2 * jnp.minimum(m, wide)

    def share(pos, m):
        return jnp.where(m < wide, pos, lax.rem(pos + m, 2))

    def partner_of(m):
        return lax.rem(x + 1 - 2 * lax.rem(x + m, 2) + nx, nx)

    t_load = pltpu.make_async_copy(t_hbm, t_ref, in_sem.at[0])
    p_load = pltpu.make_async_copy(p_hbm, p_ref, in_sem.at[1])
    p_load.start()
    t_load.start()

    barrier = pltpu.get_barrier_semaphore()

    def greet(o, _):
        dd, yy, cc, _ = at_b(me_b + o)
        pl.semaphore_signal(barrier, inc=1, device_id=dev(depth=dd, y=yy, core=cc), device_id_type=MESH)
        return 0

    lax.fori_loop(1, nb, greet, 0)
    for o in range(1, nx):
        pl.semaphore_signal(barrier, inc=1, device_id=dev(x=lax.rem(x + o, nx)), device_id_type=MESH)
    for o in (1, nz - 1):
        dd, zz = at_z(z + o)
        pl.semaphore_signal(barrier, inc=1, device_id=dev(depth=dd, zl=zz), device_id_type=MESH)
    qs[...] = q_ref[...].T
    qbuf[me_b] = qs[pl.ds(pl.multiple_of(rk * piece, 8), piece), :]
    p_load.wait()
    pl.semaphore_wait(barrier, nb - 1 + nx - 1 + 2)

    def q_copy(o):
        dd, yy, cc, r = at_b(me_b + o)
        src = qs.at[pl.ds(pl.multiple_of(r * piece, 8), piece)]
        return remote(src, qbuf.at[me_b], q_send.at[o], q_recv.at[o], dev(depth=dd, y=yy, core=cc))

    def q_arrival(o):
        src = lax.rem(me_b + nb - o, nb)
        dd, yy, cc, _ = at_b(src)
        return remote(qbuf.at[src], qbuf.at[src], q_send.at[o], q_recv.at[o], dev(depth=dd, y=yy, core=cc))

    def e_rows(j, pos):
        m = lax.div(j, 2)
        start = (2 * (base(m) + share(pos, m)) + lax.rem(j, 2)) * unit
        return p_ref.at[:, pl.ds(pl.multiple_of(start, unit), unit)]

    def e_copy(j, o):
        to = lax.rem(x + o, nx)
        return remote(e_rows(j, to), gat.at[j, d, x, zl], e_send.at[j, o], e_recv.at[j, o], dev(x=to))

    def e_arrival(j, o):
        src = lax.rem(x + nx - o, nx)
        ref = gat.at[j, d, src, zl]
        return remote(ref, ref, e_send.at[j, o], e_recv.at[j, o], dev(x=src))

    def e_local(j):
        return pltpu.make_async_copy(e_rows(j, x), gat.at[j, d, x, zl], e_own.at[j])

    def e_start(j):
        for o in (1, nx - 1, 2):
            e_copy(j, o).start()
        e_local(j).start()

    def e_step(j, _):
        e_start(j)
        return 0

    def q_step(o, _):
        q_copy(o).start()
        return 0

    e_start(0)
    lax.fori_loop(1, nb, q_step, 0)
    lax.fori_loop(1, min(ahead, chunks), e_step, 0)

    nlong, nshort = nz // 2, (nz - 1) // 2

    def z_parts(j, hop, far, arriving):
        sign = 1 - 2 * lax.rem(j, 2)
        step = sign if far else -sign
        index = hop - 1 if far else nlong + hop - 1
        dd, zz = at_z(z - step * (hop if arriving else hop - 1))
        to_d, to_z = at_z(z - step if arriving else z + step)
        ref = gat.at[j, dd, :, zz]
        return remote(ref, ref, z_send.at[j, index], z_recv.at[j, index], dev(depth=to_d, zl=to_z))

    def z_copy(j, hop, far):
        return z_parts(j, hop, far, False)

    def z_arrival(j, hop, far):
        return z_parts(j, hop, far, True)

    def hop(j, h):
        if h == 1:
            e_local(j).wait()
            for o in (1, nx - 1, 2):
                e_arrival(j, o).wait_recv()
        for far, count in ((True, nlong), (False, nshort)):
            if 2 <= h <= count + 1:
                z_arrival(j, h - 1, far).wait_recv()
            if h <= count:
                z_copy(j, h, far).start()

    def slot(t):
        for h in range(nlong + 1, 0, -1):
            if isinstance(t, int):
                if 0 <= t - h < chunks:
                    hop(t - h, h)
            else:
                pl.when((t - h >= 0) & (t - h < chunks))(functools.partial(hop, t - h, h))
        nxt = t + ahead - 1
        if isinstance(t, int):
            if nxt < chunks:
                e_start(nxt)
        else:
            pl.when(nxt < chunks)(functools.partial(e_start, nxt))

    ylong, yshort = ny // 2, (ny - 1) // 2
    ways = [(h, True) for h in range(1, ylong + 1)] + [(h, False) for h in range(1, yshort + 1)]

    def columns_of(e):
        return d if e == 0 else 1 - d

    def left_piece():
        def q_wait(o, _):
            q_arrival(o).wait_recv()
            return 0

        lax.fori_loop(1, nb, q_wait, 0)
        for b in range(nb):
            qrow[:, b * qk:(b + 1) * qk] = qbuf[b]
        t_load.wait()
        qh, ql = split(qrow[...])
        th, tl = split(t_ref[...])
        lf[d, x, rk] = dot(qh, th) + dot(qh, tl) + dot(ql, th)

    def depth_copy(e):
        ref = lf.at[columns_of(e), x, rk]
        return remote(ref, ref, d_send.at[0], d_recv.at[0], dev(depth=1 - d))

    def lx_copy(o, e):
        ref = lf.at[columns_of(e), x, rk]
        return remote(ref, ref, lx_send.at[o, e], lx_recv.at[o, e], dev(x=lax.rem(x + o, nx)))

    def lx_arrival(o, e):
        src = lax.rem(x + nx - o, nx)
        ref = lf.at[columns_of(e), src, rk]
        return remote(ref, ref, lx_send.at[o, e], lx_recv.at[o, e], dev(x=src))

    def y_index(h, far):
        return h - 1 if far else ylong + h - 1

    def y_step(xs, far):
        sign = 1 - 2 * lax.rem(xs, 2)
        return sign if far else -sign

    def y_parts(xs, e, h, far, arriving):
        step = y_step(xs, far)
        owner = lax.rem(y - step * (h if arriving else h - 1) + ny, ny)
        to = lax.rem((y - step if arriving else y + step) + ny, ny)
        ref = lf.at[columns_of(e), xs, owner * nc + core]
        i = y_index(h, far)
        return remote(ref, ref, y_send.at[xs, e, i], y_recv.at[xs, e, i], dev(y=to))

    def c_copy(xs, e, h, far, arriving=False):
        owner = lax.rem(y - y_step(xs, far) * h + ny, ny)
        i = 0 if h == 0 else 1 + y_index(h, far)
        ref = lf.at[columns_of(e), xs, owner * nc + (1 - core if arriving else core)]
        return remote(ref, ref, c_send.at[xs, e, i], c_recv.at[xs, e, i], dev(core=1 - core))

    def y_first(xs, e):
        for h, far in ways:
            if h == 1:
                y_parts(xs, e, 1, far, False).start()
        c_copy(xs, e, 0, True).start()

    def y_later(xs, e, h):
        for far, count in ((True, ylong), (False, yshort)):
            if 1 <= h - 1 <= count:
                y_parts(xs, e, h - 1, far, True).wait_recv()
                if h <= count:
                    y_parts(xs, e, h, far, False).start()
                c_copy(xs, e, h - 1, far).start()

    def each_xs(work):
        def step(o, _):
            work(lax.rem(x + o, nx))
            return 0
        lax.fori_loop(0, nx, step, 0)

    def left_ready(xs):
        for h, far in [(0, True)] + ways:
            for e in range(2):
                c_copy(xs, e, h, far, arriving=True).wait_recv()
        for b in range(nd):
            high, low = split(lf[b, xs].reshape(rows, half))
            lhi[xs, :, b * half:(b + 1) * half] = high
            llo[xs, :, b * half:(b + 1) * half] = low

    def piece_event():
        left_piece()
        depth_copy(0).start()
        for o in (1, nx - 1, 2):
            lx_copy(o, 0).start()
        y_first(x, 0)

    def lx_event(e):
        for o in (1, nx - 1, 2):
            lx_arrival(o, e).wait_recv()
            y_first(lax.rem(x + nx - o, nx), e)

    def depth_event():
        depth_copy(1).wait_recv()
        for o in (1, nx - 1, 2):
            lx_copy(o, 1).start()
        y_first(x, 1)

    def y_event(e, h):
        each_xs(lambda xs: y_later(xs, e, h))

    def own_copy(m):
        start = (base(m) + share(x, m)) * 2 * unit
        dst = out_ref.at[:, pl.ds(pl.multiple_of(start, 2 * unit), 2 * unit)]
        return pltpu.make_async_copy(obuf.at[base(m)], dst, o_own.at[m])

    def ship(m, s, to, arriving=False):
        start = (base(m) + share(to if arriving else x, m)) * 2 * unit
        dst = out_ref.at[:, pl.ds(pl.multiple_of(start, 2 * unit), 2 * unit)]
        i = base(m) + s
        return remote(obuf.at[i], dst, o_send.at[i], o_recv.at[i], dev(x=to))

    def product(i, xs):
        obuf[i] = (dot(lhi[xs], phi[...]) + dot(lhi[xs], plo[...])) + dot(llo[xs], phi[...])

    def compute(m):
        for part in range(2):
            high, low = split(gat[2 * m + part].reshape(k_full, unit))
            phi[:, part * unit:(part + 1) * unit] = high
            plo[:, part * unit:(part + 1) * unit] = low

        def send_one(s, _):
            to = jnp.where(m < wide, lax.rem(x + s, nx), partner_of(m))
            product(base(m) + s, to)
            ship(m, s, to).start()
            return 0

        lax.fori_loop(1, jnp.where(m < wide, nx, 2), send_one, 0)
        product(base(m), x)
        own_copy(m).start()

    slot(1)
    slot(2)
    piece_event()
    slot(3)
    slot(4)
    lx_event(0)
    depth_event()
    slot(5)
    lx_event(1)
    y_event(0, 2)
    slot(6)
    y_event(1, 2)
    slot(7)
    y_event(0, 3)
    slot(8)
    y_event(1, 3)
    each_xs(left_ready)

    def caught_up(m, _):
        compute(m)
        return 0

    def body(m, _):
        slot(2 * m + 5)
        slot(2 * m + 6)
        compute(m)
        return 0

    lax.fori_loop(0, min(2, pairs), caught_up, 0)
    lax.fori_loop(2, pairs, body, 0)

    def finish(j, _):
        for o in range(1, nx):
            e_copy(j, o).wait_send()
        for h in range(1, nlong + 1):
            z_copy(j, h, True).wait_send()
        for h in range(1, nshort + 1):
            z_copy(j, h, False).wait_send()
        return 0

    lax.fori_loop(0, chunks, finish, 0)

    def q_finish(o, _):
        q_copy(o).wait_send()
        return 0

    lax.fori_loop(1, nb, q_finish, 0)
    depth_copy(0).wait_send()
    for e in range(2):
        for o in range(1, nx):
            lx_copy(o, e).wait_send()

    def y_finish(xs):
        for e in range(2):
            c_copy(xs, e, 0, True).wait_send()
            for h, far in ways:
                c_copy(xs, e, h, far).wait_send()
                y_parts(xs, e, h, far, False).wait_send()

    each_xs(y_finish)

    def out_finish(m, _):
        own_copy(m).wait()

        def one(s, _):
            ship(m, s, jnp.where(m < wide, lax.rem(x + s, nx), partner_of(m))).wait_send()
            src = jnp.where(m < wide, lax.rem(x + nx - s, nx), partner_of(m))
            ship(m, s, src, arriving=True).wait_recv()
            return 0

        lax.fori_loop(1, jnp.where(m < wide, nx, 2), one, 0)
        return 0

    lax.fori_loop(0, pairs, out_finish, 0)


def per_device(dims, unit, wide, q_slab, triangle, panel_q):
    nd, ny, nc, nx, nzl = dims
    nz, nr, nb = nd * nzl, ny * nc, nd * ny * nc
    rows, qk = q_slab.shape
    k_full, half = triangle.shape
    out_cols, narrow = panel_q.shape
    blocks = out_cols // (2 * unit)
    pairs = (blocks - 4 * wide) // 2 + wide
    chunks = 2 * pairs
    dma = pltpu.SemaphoreType.DMA
    far = pl.BlockSpec(memory_space=pl.ANY)
    return pl.pallas_call(
        functools.partial(kernel, dims, unit, (wide, pairs)),
        out_shape=jax.ShapeDtypeStruct((rows, out_cols), F32),
        in_specs=[pl.BlockSpec(memory_space=pltpu.VMEM), far, far],
        out_specs=far,
        scratch_shapes=[
            pltpu.VMEM((rows, qk), F32),
            pltpu.VMEM((k_full, half), F32),
            pltpu.VMEM((narrow, out_cols), F32),
            pltpu.VMEM((nb, rows // nr, qk), F32),
            pltpu.VMEM((rows // nr, k_full), F32),
            pltpu.VMEM((nd, nx, nr, rows // nr, half), F32),
            pltpu.VMEM((nx, rows, k_full), BF16),
            pltpu.VMEM((nx, rows, k_full), BF16),
            pltpu.VMEM((chunks, nd, nx, nzl, narrow, unit), F32),
            pltpu.VMEM((k_full, 2 * unit), BF16),
            pltpu.VMEM((k_full, 2 * unit), BF16),
            pltpu.VMEM((blocks, rows, 2 * unit), F32),
            dma((2,)),
            dma((nb,)), dma((nb,)),
            dma((chunks, nx)), dma((chunks, nx)), dma((chunks,)),
            dma((chunks, nz)), dma((chunks, nz)),
            dma((1,)), dma((1,)),
            dma((nx, 2)), dma((nx, 2)),
            dma((nx, 2, ny)), dma((nx, 2, ny)),
            dma((nx, 2, ny)), dma((nx, 2, ny)),
            dma((pairs,)), dma((blocks,)), dma((blocks,)),
        ],
        compiler_params=pltpu.CompilerParams(
            collective_id=0, has_side_effects=True, vmem_limit_bytes=60 * 1024 * 1024
        ),
    )(q_slab.T, triangle, panel_q.T)


def build(mesh, dims, unit, wide=1):
    torus = Mesh(mesh.devices.reshape(dims), AXES)
    slab = ("x", "zl")
    row = ("y", "core")
    in_specs = (P(slab, ("depth",) + row), P(None, "depth"), P(row, ("depth",) + slab))
    return jax.shard_map(
        functools.partial(per_device, dims, unit, wide),
        mesh=torus, in_specs=in_specs, out_specs=P(slab, row), check_vma=False)


def solution(mesh):
    return build(mesh, (mesh.shape["depth"], 4, 2, 4, 4), 128)
```

```python
import functools

import jax
import jax.numpy as jnp
from jax import lax
from jax.experimental import pallas as pl
from jax.experimental.pallas import tpu as pltpu
from jax.sharding import Mesh
from jax.sharding import PartitionSpec as P

AXES = ("depth", "y", "core", "x", "zl")
MESH = pl.DeviceIdType.MESH
F32, BF16 = jnp.float32, jnp.bfloat16


def split(value):
    high = value.astype(BF16)
    return high, (value - high.astype(F32)).astype(BF16)


def dot(a, b):
    return jnp.dot(a, b, preferred_element_type=F32)


def kernel(dims, unit, plan, q_ref, t_hbm, p_hbm, out_ref,
           qs, t_ref, p_ref, qbuf, qrow, lf, lhi, llo, gat, phi, plo, obuf, in_sem,
           q_send, q_recv, e_send, e_recv, e_own, z_send, z_recv,
           d_send, d_recv, lx_send, lx_recv, y_send, y_recv,
           c_send, c_recv, o_own, o_send, o_recv):
    wide, pairs = plan
    nd, ny, nc, nx, nzl = dims
    nz = nd * nzl
    nr = ny * nc
    nb = nd * nr
    d, y, core, x, zl = (lax.axis_index(a) for a in AXES)
    z = d * nzl + zl
    rk = y * nc + core
    me_b = d * nr + rk
    chunks = 2 * pairs
    ahead = 8
    piece = lf.shape[3]
    half = lf.shape[4]
    k_full = nd * half
    rows = nr * piece
    qk = qs.shape[1]

    def dev(**over):
        return tuple(over.get(a, v) for a, v in zip(AXES, (d, y, core, x, zl)))

    def at_z(pos):
        pos = lax.rem(pos + nz, nz)
        return lax.div(pos, nzl), lax.rem(pos, nzl)

    def at_b(pos):
        pos = lax.rem(pos, nb)
        dd, r = lax.div(pos, nr), lax.rem(pos, nr)
        return dd, lax.div(r, nc), lax.rem(r, nc), r

    def remote(src, dst, send, recv, to):
        return pltpu.make_async_remote_copy(
            src_ref=src, dst_ref=dst, send_sem=send, recv_sem=recv,
            device_id=to, device_id_type=MESH)

    def base(m):
        return 2 * m + 2 * jnp.minimum(lax.div(m, 2), wide)

    def is_wide(m):
        return (lax.rem(m, 2) == 1) & (m < 2 * wide)

    def role(pos, m):
        return lax.rem(pos + lax.div(m, 2) + lax.rem(m, 2), 2)

    def share(pos, m):
        return jnp.where(is_wide(m), pos, role(pos, m))

    def partner_of(m):
        return lax.rem(x + 1 - 2 * role(x, m) + nx, nx)

    def receivers(m):
        return jnp.where(is_wide(m), nx - 1, 1)

    def receiver(m, s):
        return jnp.where(is_wide(m), lax.rem(x + s, nx), partner_of(m))

    def sender(m, s):
        return jnp.where(is_wide(m), lax.rem(x + nx - s, nx), partner_of(m))

    t_load = pltpu.make_async_copy(t_hbm, t_ref, in_sem.at[0])
    p_load = pltpu.make_async_copy(p_hbm, p_ref, in_sem.at[1])
    p_load.start()
    t_load.start()

    barrier = pltpu.get_barrier_semaphore()

    def greet(o, _):
        dd, yy, cc, _ = at_b(me_b + o)
        pl.semaphore_signal(barrier, inc=1, device_id=dev(depth=dd, y=yy, core=cc), device_id_type=MESH)
        return 0

    lax.fori_loop(1, nb, greet, 0)
    for o in range(1, nx):
        pl.semaphore_signal(barrier, inc=1, device_id=dev(x=lax.rem(x + o, nx)), device_id_type=MESH)
    for o in (1, nz - 1):
        dd, zz = at_z(z + o)
        pl.semaphore_signal(barrier, inc=1, device_id=dev(depth=dd, zl=zz), device_id_type=MESH)
    qs[...] = q_ref[...].T
    qbuf[me_b] = qs[pl.ds(pl.multiple_of(rk * piece, 8), piece), :]
    p_load.wait()
    pl.semaphore_wait(barrier, nb - 1 + nx - 1 + 2)

    def q_copy(o):
        dd, yy, cc, r = at_b(me_b + o)
        src = qs.at[pl.ds(pl.multiple_of(r * piece, 8), piece)]
        return remote(src, qbuf.at[me_b], q_send.at[o], q_recv.at[o], dev(depth=dd, y=yy, core=cc))

    def q_arrival(o):
        src = lax.rem(me_b + nb - o, nb)
        dd, yy, cc, _ = at_b(src)
        return remote(qbuf.at[src], qbuf.at[src], q_send.at[o], q_recv.at[o], dev(depth=dd, y=yy, core=cc))

    def e_rows(j, pos):
        m = lax.div(j, 2)
        start = (2 * (base(m) + share(pos, m)) + lax.rem(j, 2)) * unit
        return p_ref.at[:, pl.ds(pl.multiple_of(start, unit), unit)]

    def e_copy(j, o):
        to = lax.rem(x + o, nx)
        return remote(e_rows(j, to), gat.at[j, d, x, zl], e_send.at[j, o], e_recv.at[j, o], dev(x=to))

    def e_arrival(j, o):
        src = lax.rem(x + nx - o, nx)
        ref = gat.at[j, d, src, zl]
        return remote(ref, ref, e_send.at[j, o], e_recv.at[j, o], dev(x=src))

    def e_local(j):
        return pltpu.make_async_copy(e_rows(j, x), gat.at[j, d, x, zl], e_own.at[j])

    def e_start(j):
        for o in (1, nx - 1, 2):
            e_copy(j, o).start()
        e_local(j).start()

    def e_step(j, _):
        e_start(j)
        return 0

    def q_step(o, _):
        q_copy(o).start()
        return 0

    e_start(0)
    lax.fori_loop(1, nb, q_step, 0)
    lax.fori_loop(1, min(ahead, chunks), e_step, 0)

    nlong, nshort = nz // 2, (nz - 1) // 2

    def z_parts(j, hop, far, arriving):
        sign = 1 - 2 * lax.rem(j, 2)
        step = sign if far else -sign
        index = hop - 1 if far else nlong + hop - 1
        dd, zz = at_z(z - step * (hop if arriving else hop - 1))
        to_d, to_z = at_z(z - step if arriving else z + step)
        ref = gat.at[j, dd, :, zz]
        return remote(ref, ref, z_send.at[j, index], z_recv.at[j, index], dev(depth=to_d, zl=to_z))

    def z_copy(j, hop, far):
        return z_parts(j, hop, far, False)

    def z_arrival(j, hop, far):
        return z_parts(j, hop, far, True)

    def hop(j, h):
        if h == 1:
            e_local(j).wait()
            for o in (1, nx - 1, 2):
                e_arrival(j, o).wait_recv()
        for far, count in ((True, nlong), (False, nshort)):
            if 2 <= h <= count + 1:
                z_arrival(j, h - 1, far).wait_recv()
            if h <= count:
                z_copy(j, h, far).start()

    def step(g, h):
        for c in range(4):
            hop(4 * g + c, h)

    ylong, yshort = ny // 2, (ny - 1) // 2
    ways = [(h, True) for h in range(1, ylong + 1)] + [(h, False) for h in range(1, yshort + 1)]

    def columns_of(e):
        return d if e == 0 else 1 - d

    def left_piece():
        def q_wait(o, _):
            q_arrival(o).wait_recv()
            return 0

        lax.fori_loop(1, nb, q_wait, 0)
        for b in range(nb):
            qrow[:, b * qk:(b + 1) * qk] = qbuf[b]
        t_load.wait()
        qh, ql = split(qrow[...])
        th, tl = split(t_ref[...])
        lf[d, x, rk] = dot(qh, th) + dot(qh, tl) + dot(ql, th)

    def depth_copy(e):
        ref = lf.at[columns_of(e), x, rk]
        return remote(ref, ref, d_send.at[0], d_recv.at[0], dev(depth=1 - d))

    def lx_copy(o, e):
        ref = lf.at[columns_of(e), x, rk]
        return remote(ref, ref, lx_send.at[o, e], lx_recv.at[o, e], dev(x=lax.rem(x + o, nx)))

    def lx_arrival(o, e):
        src = lax.rem(x + nx - o, nx)
        ref = lf.at[columns_of(e), src, rk]
        return remote(ref, ref, lx_send.at[o, e], lx_recv.at[o, e], dev(x=src))

    def y_index(h, far):
        return h - 1 if far else ylong + h - 1

    def y_step(xs, far):
        sign = 1 - 2 * lax.rem(xs, 2)
        return sign if far else -sign

    def y_parts(xs, e, h, far, arriving):
        step = y_step(xs, far)
        owner = lax.rem(y - step * (h if arriving else h - 1) + ny, ny)
        to = lax.rem((y - step if arriving else y + step) + ny, ny)
        ref = lf.at[columns_of(e), xs, owner * nc + core]
        i = y_index(h, far)
        return remote(ref, ref, y_send.at[xs, e, i], y_recv.at[xs, e, i], dev(y=to))

    def c_copy(xs, e, h, far, arriving=False):
        owner = lax.rem(y - y_step(xs, far) * h + ny, ny)
        i = 0 if h == 0 else 1 + y_index(h, far)
        ref = lf.at[columns_of(e), xs, owner * nc + (1 - core if arriving else core)]
        return remote(ref, ref, c_send.at[xs, e, i], c_recv.at[xs, e, i], dev(core=1 - core))

    def y_first(xs, e):
        for h, far in ways:
            if h == 1:
                y_parts(xs, e, 1, far, False).start()
        c_copy(xs, e, 0, True).start()

    def y_later(xs, e, h):
        for far, count in ((True, ylong), (False, yshort)):
            if 1 <= h - 1 <= count:
                y_parts(xs, e, h - 1, far, True).wait_recv()
                if h <= count:
                    y_parts(xs, e, h, far, False).start()
                c_copy(xs, e, h - 1, far).start()

    def left_ready(xs):
        for h, far in [(0, True)] + ways:
            for e in range(2):
                c_copy(xs, e, h, far, arriving=True).wait_recv()
        for b in range(nd):
            high, low = split(lf[b, xs].reshape(rows, half))
            lhi[xs, :, b * half:(b + 1) * half] = high
            llo[xs, :, b * half:(b + 1) * half] = low

    def piece_event():
        left_piece()
        depth_copy(0).start()
        for o in (1, nx - 1, 2):
            lx_copy(o, 0).start()
        y_first(x, 0)

    def lx_event(o, e):
        lx_arrival(o, e).wait_recv()
        y_first(lax.rem(x + nx - o, nx), e)

    def depth_event():
        depth_copy(1).wait_recv()
        for o in (1, nx - 1, 2):
            lx_copy(o, 1).start()

    near = (lax.rem(x + nx - 1, nx), lax.rem(x + 1, nx))
    across = lax.rem(x + 2, nx)

    def own_copy(m):
        start = (base(m) + share(x, m)) * 2 * unit
        dst = out_ref.at[:, pl.ds(pl.multiple_of(start, 2 * unit), 2 * unit)]
        return pltpu.make_async_copy(obuf.at[base(m)], dst, o_own.at[m])

    def ship(m, s, to, arriving=False):
        start = (base(m) + share(to if arriving else x, m)) * 2 * unit
        dst = out_ref.at[:, pl.ds(pl.multiple_of(start, 2 * unit), 2 * unit)]
        i = base(m) + s
        return remote(obuf.at[i], dst, o_send.at[i], o_recv.at[i], dev(x=to))

    def prepare(m):
        for part in range(2):
            high, low = split(gat[2 * m + part].reshape(k_full, unit))
            phi[lax.rem(m, 2), :, part * unit:(part + 1) * unit] = high
            plo[lax.rem(m, 2), :, part * unit:(part + 1) * unit] = low

    def product(m, i, xs):
        high, low = phi[lax.rem(m, 2)], plo[lax.rem(m, 2)]
        obuf[base(m) + i] = (dot(lhi[xs], high) + dot(lhi[xs], low)) + dot(llo[xs], high)

    def compute_others(m):
        prepare(m)

        def one(s, _):
            to = receiver(m, s)
            product(m, s, to)
            ship(m, s, to).start()
            return 0

        lax.fori_loop(1, receivers(m) + 1, one, 0)

    def compute_own(m):
        product(m, 0, x)
        own_copy(m).start()

    groups = chunks // 4
    step(0, 1)
    piece_event()
    step(0, 2)
    for o in (1, nx - 1):
        lx_event(o, 0)
    depth_event()
    step(0, 3)
    lax.fori_loop(ahead, chunks, e_step, 0)
    for xs in near:
        y_later(xs, 0, 2)
    for o in (1, nx - 1):
        lx_event(o, 1)
    step(0, 4)
    step(1, 1)
    for xs in near:
        y_later(xs, 1, 2)
    y_first(x, 1)
    y_later(x, 0, 2)
    for e in range(2):
        lx_event(2, e)
    step(0, 5)
    step(1, 2)
    for xs in near:
        for e in range(2):
            y_later(xs, e, 3)
    for xs in near:
        left_ready(xs)
    compute_others(0)
    y_later(x, 1, 2)
    step(1, 3)
    for e in range(2):
        y_later(across, e, 2)
        y_later(x, e, 3)
    left_ready(x)
    compute_own(0)
    step(1, 4)
    step(2, 1)
    for e in range(2):
        y_later(across, e, 3)
    left_ready(across)
    compute_others(1)
    compute_own(1)
    for g in range(2, groups):
        if g > 2:
            step(g - 1, 4)
            step(g, 1)
        step(g - 1, 5)
        step(g, 2)
        compute_others(2 * g - 2)
        compute_own(2 * g - 2)
        step(g, 3)
        compute_others(2 * g - 1)
        compute_own(2 * g - 1)
    step(groups - 1, 4)
    step(groups - 1, 5)
    for m in (2 * groups - 2, 2 * groups - 1):
        compute_others(m)
    for m in (2 * groups - 2, 2 * groups - 1):
        compute_own(m)

    def finish(j, _):
        for o in range(1, nx):
            e_copy(j, o).wait_send()
        for h in range(1, nlong + 1):
            z_copy(j, h, True).wait_send()
        for h in range(1, nshort + 1):
            z_copy(j, h, False).wait_send()
        return 0

    lax.fori_loop(0, chunks, finish, 0)

    def q_finish(o, _):
        q_copy(o).wait_send()
        return 0

    lax.fori_loop(1, nb, q_finish, 0)
    depth_copy(0).wait_send()
    for e in range(2):
        for o in range(1, nx):
            lx_copy(o, e).wait_send()

    def y_finish(xs, _):
        for e in range(2):
            c_copy(xs, e, 0, True).wait_send()
            for h, far in ways:
                c_copy(xs, e, h, far).wait_send()
                y_parts(xs, e, h, far, False).wait_send()
        return 0

    lax.fori_loop(0, nx, y_finish, 0)

    def out_finish(m, _):
        own_copy(m).wait()

        def one(s, _):
            ship(m, s, receiver(m, s)).wait_send()
            ship(m, s, sender(m, s), arriving=True).wait_recv()
            return 0

        lax.fori_loop(1, receivers(m) + 1, one, 0)
        return 0

    lax.fori_loop(0, pairs, out_finish, 0)


def per_device(dims, unit, wide, q_slab, triangle, panel_q):
    nd, ny, nc, nx, nzl = dims
    nz, nr, nb = nd * nzl, ny * nc, nd * ny * nc
    rows, qk = q_slab.shape
    k_full, half = triangle.shape
    out_cols, narrow = panel_q.shape
    blocks = out_cols // (2 * unit)
    pairs = (blocks - 4 * wide) // 2 + wide
    chunks = 2 * pairs
    dma = pltpu.SemaphoreType.DMA
    far = pl.BlockSpec(memory_space=pl.ANY)
    return pl.pallas_call(
        functools.partial(kernel, dims, unit, (wide, pairs)),
        out_shape=jax.ShapeDtypeStruct((rows, out_cols), F32),
        in_specs=[pl.BlockSpec(memory_space=pltpu.VMEM), far, far],
        out_specs=far,
        scratch_shapes=[
            pltpu.VMEM((rows, qk), F32),
            pltpu.VMEM((k_full, half), F32),
            pltpu.VMEM((narrow, out_cols), F32),
            pltpu.VMEM((nb, rows // nr, qk), F32),
            pltpu.VMEM((rows // nr, k_full), F32),
            pltpu.VMEM((nd, nx, nr, rows // nr, half), F32),
            pltpu.VMEM((nx, rows, k_full), BF16),
            pltpu.VMEM((nx, rows, k_full), BF16),
            pltpu.VMEM((chunks, nd, nx, nzl, narrow, unit), F32),
            pltpu.VMEM((2, k_full, 2 * unit), BF16),
            pltpu.VMEM((2, k_full, 2 * unit), BF16),
            pltpu.VMEM((blocks, rows, 2 * unit), F32),
            dma((2,)),
            dma((nb,)), dma((nb,)),
            dma((chunks, nx)), dma((chunks, nx)), dma((chunks,)),
            dma((chunks, nz)), dma((chunks, nz)),
            dma((1,)), dma((1,)),
            dma((nx, 2)), dma((nx, 2)),
            dma((nx, 2, ny)), dma((nx, 2, ny)),
            dma((nx, 2, ny)), dma((nx, 2, ny)),
            dma((pairs,)), dma((blocks,)), dma((blocks,)),
        ],
        compiler_params=pltpu.CompilerParams(
            collective_id=0, has_side_effects=True, vmem_limit_bytes=57 * 1024 * 1024
        ),
    )(q_slab.T, triangle, panel_q.T)


def build(mesh, dims, unit, wide=2):
    torus = Mesh(mesh.devices.reshape(dims), AXES)
    slab = ("x", "zl")
    row = ("y", "core")
    in_specs = (P(slab, ("depth",) + row), P(None, "depth"), P(row, ("depth",) + slab))
    return jax.shard_map(
        functools.partial(per_device, dims, unit, wide),
        mesh=torus, in_specs=in_specs, out_specs=P(slab, row), check_vma=False)


def solution(mesh):
    return build(mesh, (mesh.shape["depth"], 4, 2, 4, 4), 128)
```

```python
import functools

import jax
import jax.numpy as jnp
from jax import lax
from jax.experimental import pallas as pl
from jax.experimental.pallas import tpu as pltpu
from jax.sharding import Mesh
from jax.sharding import PartitionSpec as P

AXES = ("depth", "y", "core", "x", "zl")
MESH = pl.DeviceIdType.MESH
F32, BF16 = jnp.float32, jnp.bfloat16


def split(value):
    high = value.astype(BF16)
    return high, (value - high.astype(F32)).astype(BF16)


def dot(a, b):
    return jnp.dot(a, b, preferred_element_type=F32)


def kernel(dims, unit, plan, q_ref, t_hbm, p_hbm, out_ref,
           qs, t_ref, p_ref, qbuf, qrow, lf, lhi, llo, gat, phi, plo, obuf, in_sem,
           q_send, q_recv, e_send, e_recv, e_own, z_send, z_recv,
           d_send, d_recv, lx_send, lx_recv, y_send, y_recv,
           c_send, c_recv, o_own, o_send, o_recv):
    wide, pairs = plan
    nd, ny, nc, nx, nzl = dims
    nz = nd * nzl
    nr = ny * nc
    nb = nd * nr
    d, y, core, x, zl = (lax.axis_index(a) for a in AXES)
    z = d * nzl + zl
    rk = y * nc + core
    me_b = d * nr + rk
    chunks = 2 * pairs
    ahead = 8
    piece = lf.shape[3]
    half = lf.shape[4]
    k_full = nd * half
    rows = nr * piece
    qk = qs.shape[1]

    def dev(**over):
        return tuple(over.get(a, v) for a, v in zip(AXES, (d, y, core, x, zl)))

    def at_z(pos):
        pos = lax.rem(pos + nz, nz)
        return lax.div(pos, nzl), lax.rem(pos, nzl)

    def at_b(pos):
        pos = lax.rem(pos, nb)
        dd, r = lax.div(pos, nr), lax.rem(pos, nr)
        return dd, lax.div(r, nc), lax.rem(r, nc), r

    def remote(src, dst, send, recv, to):
        return pltpu.make_async_remote_copy(
            src_ref=src, dst_ref=dst, send_sem=send, recv_sem=recv,
            device_id=to, device_id_type=MESH)

    def wide_before(m):
        return jnp.clip(m - 2, 0, wide)

    def base(m):
        return 2 * m + 2 * wide_before(m)

    def is_wide(m):
        return (m >= 2) & (m < 2 + wide)

    def role(pos, m):
        return lax.rem(pos + m + wide_before(m), 2)

    def share(pos, m):
        return jnp.where(is_wide(m), pos, role(pos, m))

    def partner_of(m):
        return lax.rem(x + 1 - 2 * role(x, m) + nx, nx)

    def receivers(m):
        return jnp.where(is_wide(m), nx - 1, 1)

    def receiver(m, s):
        return jnp.where(is_wide(m), lax.rem(x + s, nx), partner_of(m))

    def sender(m, s):
        return jnp.where(is_wide(m), lax.rem(x + nx - s, nx), partner_of(m))

    t_load = pltpu.make_async_copy(t_hbm, t_ref, in_sem.at[0])
    p_load = pltpu.make_async_copy(p_hbm, p_ref, in_sem.at[1])
    p_load.start()
    t_load.start()

    barrier = pltpu.get_barrier_semaphore()

    def greet(o, _):
        dd, yy, cc, _ = at_b(me_b + o)
        pl.semaphore_signal(barrier, inc=1, device_id=dev(depth=dd, y=yy, core=cc), device_id_type=MESH)
        return 0

    lax.fori_loop(1, nb, greet, 0)
    for o in range(1, nx):
        pl.semaphore_signal(barrier, inc=1, device_id=dev(x=lax.rem(x + o, nx)), device_id_type=MESH)
    for o in (1, nz - 1):
        dd, zz = at_z(z + o)
        pl.semaphore_signal(barrier, inc=1, device_id=dev(depth=dd, zl=zz), device_id_type=MESH)
    qs[...] = q_ref[...].T
    qbuf[me_b] = qs[pl.ds(pl.multiple_of(rk * piece, 8), piece), :]
    p_load.wait()
    pl.semaphore_wait(barrier, nb - 1 + nx - 1 + 2)

    def q_copy(o):
        dd, yy, cc, r = at_b(me_b + o)
        src = qs.at[pl.ds(pl.multiple_of(r * piece, 8), piece)]
        return remote(src, qbuf.at[me_b], q_send.at[o], q_recv.at[o], dev(depth=dd, y=yy, core=cc))

    def q_arrival(o):
        src = lax.rem(me_b + nb - o, nb)
        dd, yy, cc, _ = at_b(src)
        return remote(qbuf.at[src], qbuf.at[src], q_send.at[o], q_recv.at[o], dev(depth=dd, y=yy, core=cc))

    def e_rows(j, pos):
        m = lax.div(j, 2)
        start = (2 * (base(m) + share(pos, m)) + lax.rem(j, 2)) * unit
        return p_ref.at[:, pl.ds(pl.multiple_of(start, unit), unit)]

    def e_copy(j, o):
        to = lax.rem(x + o, nx)
        return remote(e_rows(j, to), gat.at[j, d, x, zl], e_send.at[j, o], e_recv.at[j, o], dev(x=to))

    def e_arrival(j, o):
        src = lax.rem(x + nx - o, nx)
        ref = gat.at[j, d, src, zl]
        return remote(ref, ref, e_send.at[j, o], e_recv.at[j, o], dev(x=src))

    def e_local(j):
        return pltpu.make_async_copy(e_rows(j, x), gat.at[j, d, x, zl], e_own.at[j])

    def e_start(j):
        for o in (1, nx - 1, 2):
            e_copy(j, o).start()
        e_local(j).start()

    def e_step(j, _):
        e_start(j)
        return 0

    def q_step(o, _):
        q_copy(o).start()
        return 0

    e_start(0)
    lax.fori_loop(1, nb, q_step, 0)
    lax.fori_loop(1, min(ahead, chunks), e_step, 0)

    nlong, nshort = nz // 2, (nz - 1) // 2

    def z_parts(j, hop, far, arriving):
        sign = 1 - 2 * lax.rem(j, 2)
        step = sign if far else -sign
        index = hop - 1 if far else nlong + hop - 1
        dd, zz = at_z(z - step * (hop if arriving else hop - 1))
        to_d, to_z = at_z(z - step if arriving else z + step)
        ref = gat.at[j, dd, :, zz]
        return remote(ref, ref, z_send.at[j, index], z_recv.at[j, index], dev(depth=to_d, zl=to_z))

    def z_copy(j, hop, far):
        return z_parts(j, hop, far, False)

    def z_arrival(j, hop, far):
        return z_parts(j, hop, far, True)

    def hop(j, h):
        if h == 1:
            e_local(j).wait()
            for o in (1, nx - 1, 2):
                e_arrival(j, o).wait_recv()
        for far, count in ((True, nlong), (False, nshort)):
            if 2 <= h <= count + 1:
                z_arrival(j, h - 1, far).wait_recv()
            if h <= count:
                z_copy(j, h, far).start()

    def step(g, h):
        for j in range(max(4 * g - 2, 0), 4 * g + 2):
            hop(j, h)

    ylong, yshort = ny // 2, (ny - 1) // 2
    ways = [(h, True) for h in range(1, ylong + 1)] + [(h, False) for h in range(1, yshort + 1)]

    def columns_of(e):
        return d if e == 0 else 1 - d

    def left_piece():
        def q_wait(o, _):
            q_arrival(o).wait_recv()
            return 0

        lax.fori_loop(1, nb, q_wait, 0)
        for b in range(nb):
            qrow[:, b * qk:(b + 1) * qk] = qbuf[b]
        t_load.wait()
        qh, ql = split(qrow[...])
        th, tl = split(t_ref[...])
        lf[d, x, rk] = dot(qh, th) + dot(qh, tl) + dot(ql, th)

    def depth_copy(e):
        ref = lf.at[columns_of(e), x, rk]
        return remote(ref, ref, d_send.at[0], d_recv.at[0], dev(depth=1 - d))

    def lx_copy(o, e):
        ref = lf.at[columns_of(e), x, rk]
        return remote(ref, ref, lx_send.at[o, e], lx_recv.at[o, e], dev(x=lax.rem(x + o, nx)))

    def lx_arrival(o, e):
        src = lax.rem(x + nx - o, nx)
        ref = lf.at[columns_of(e), src, rk]
        return remote(ref, ref, lx_send.at[o, e], lx_recv.at[o, e], dev(x=src))

    def y_index(h, far):
        return h - 1 if far else ylong + h - 1

    def y_step(xs, far):
        sign = 1 - 2 * lax.rem(xs, 2)
        return sign if far else -sign

    def y_parts(xs, e, h, far, arriving):
        step = y_step(xs, far)
        owner = lax.rem(y - step * (h if arriving else h - 1) + ny, ny)
        to = lax.rem((y - step if arriving else y + step) + ny, ny)
        ref = lf.at[columns_of(e), xs, owner * nc + core]
        i = y_index(h, far)
        return remote(ref, ref, y_send.at[xs, e, i], y_recv.at[xs, e, i], dev(y=to))

    def c_copy(xs, e, h, far, arriving=False):
        owner = lax.rem(y - y_step(xs, far) * h + ny, ny)
        i = 0 if h == 0 else 1 + y_index(h, far)
        ref = lf.at[columns_of(e), xs, owner * nc + (1 - core if arriving else core)]
        return remote(ref, ref, c_send.at[xs, e, i], c_recv.at[xs, e, i], dev(core=1 - core))

    def y_first(xs, e):
        for h, far in ways:
            if h == 1:
                y_parts(xs, e, 1, far, False).start()
        c_copy(xs, e, 0, True).start()

    def y_later(xs, e, h):
        for far, count in ((True, ylong), (False, yshort)):
            if 1 <= h - 1 <= count:
                y_parts(xs, e, h - 1, far, True).wait_recv()
                if h <= count:
                    y_parts(xs, e, h, far, False).start()
                c_copy(xs, e, h - 1, far).start()

    def left_ready(xs):
        for h, far in [(0, True)] + ways:
            for e in range(2):
                c_copy(xs, e, h, far, arriving=True).wait_recv()
        for b in range(nd):
            high, low = split(lf[b, xs].reshape(rows, half))
            lhi[xs, :, b * half:(b + 1) * half] = high
            llo[xs, :, b * half:(b + 1) * half] = low

    def piece_event():
        left_piece()
        depth_copy(0).start()
        for o in (1, nx - 1, 2):
            lx_copy(o, 0).start()
        y_first(x, 0)

    def lx_event(o, e):
        lx_arrival(o, e).wait_recv()
        y_first(lax.rem(x + nx - o, nx), e)

    def depth_event():
        depth_copy(1).wait_recv()
        for o in (1, nx - 1, 2):
            lx_copy(o, 1).start()

    near = (lax.rem(x + nx - 1, nx), lax.rem(x + 1, nx))
    across = lax.rem(x + 2, nx)

    def own_copy(m):
        start = (base(m) + share(x, m)) * 2 * unit
        dst = out_ref.at[:, pl.ds(pl.multiple_of(start, 2 * unit), 2 * unit)]
        return pltpu.make_async_copy(obuf.at[base(m)], dst, o_own.at[m])

    def ship(m, s, to, arriving=False):
        start = (base(m) + share(to if arriving else x, m)) * 2 * unit
        dst = out_ref.at[:, pl.ds(pl.multiple_of(start, 2 * unit), 2 * unit)]
        i = base(m) + s
        return remote(obuf.at[i], dst, o_send.at[i], o_recv.at[i], dev(x=to))

    def prepare(m):
        for part in range(2):
            high, low = split(gat[2 * m + part].reshape(k_full, unit))
            phi[lax.rem(m, 4), :, part * unit:(part + 1) * unit] = high
            plo[lax.rem(m, 4), :, part * unit:(part + 1) * unit] = low

    def product(m, i, xs):
        high, low = phi[lax.rem(m, 4)], plo[lax.rem(m, 4)]
        obuf[base(m) + i] = (dot(lhi[xs], high) + dot(lhi[xs], low)) + dot(llo[xs], high)

    def compute_others(m):
        prepare(m)

        def one(s, _):
            to = receiver(m, s)
            product(m, s, to)
            ship(m, s, to).start()
            return 0

        lax.fori_loop(1, receivers(m) + 1, one, 0)

    def compute_own(m):
        product(m, 0, x)
        own_copy(m).start()

    step(0, 1)
    step(1, 1)
    piece_event()
    step(0, 2)
    for o in (1, nx - 1):
        lx_event(o, 0)
    step(1, 2)
    depth_event()
    lax.fori_loop(ahead, chunks, e_step, 0)
    for xs in near:
        y_later(xs, 0, 2)
    step(0, 3)
    for o in (1, nx - 1):
        lx_event(o, 1)
    step(1, 3)
    for xs in near:
        y_later(xs, 1, 2)
    y_first(x, 1)
    y_later(x, 0, 2)
    for e in range(2):
        lx_event(2, e)
    step(0, 4)
    step(2, 1)
    for xs in near:
        for e in range(2):
            y_later(xs, e, 3)
    for xs in near:
        left_ready(xs)
    step(1, 4)
    step(0, 5)
    compute_others(0)
    y_later(x, 1, 2)
    for e in range(2):
        y_later(across, e, 2)
    step(2, 2)
    step(1, 5)
    compute_others(1)
    for e in range(2):
        y_later(x, e, 3)
        y_later(across, e, 3)
    step(2, 3)
    step(3, 1)
    left_ready(across)
    compute_others(2)
    step(2, 4)
    step(3, 2)
    left_ready(x)
    compute_own(0)
    compute_own(1)
    step(2, 5)
    compute_others(3)
    step(3, 3)
    compute_others(4)
    compute_own(2)
    step(3, 4)
    compute_own(3)
    compute_own(4)
    step(3, 5)
    for m in range(5, pairs):
        compute_others(m)
    for m in range(5, pairs):
        compute_own(m)

    def finish(j, _):
        for o in range(1, nx):
            e_copy(j, o).wait_send()
        for h in range(1, nlong + 1):
            z_copy(j, h, True).wait_send()
        for h in range(1, nshort + 1):
            z_copy(j, h, False).wait_send()
        return 0

    lax.fori_loop(0, chunks, finish, 0)

    def q_finish(o, _):
        q_copy(o).wait_send()
        return 0

    lax.fori_loop(1, nb, q_finish, 0)
    depth_copy(0).wait_send()
    for e in range(2):
        for o in range(1, nx):
            lx_copy(o, e).wait_send()

    def y_finish(xs, _):
        for e in range(2):
            c_copy(xs, e, 0, True).wait_send()
            for h, far in ways:
                c_copy(xs, e, h, far).wait_send()
                y_parts(xs, e, h, far, False).wait_send()
        return 0

    lax.fori_loop(0, nx, y_finish, 0)

    def out_finish(m, _):
        own_copy(m).wait()

        def one(s, _):
            ship(m, s, receiver(m, s)).wait_send()
            ship(m, s, sender(m, s), arriving=True).wait_recv()
            return 0

        lax.fori_loop(1, receivers(m) + 1, one, 0)
        return 0

    lax.fori_loop(0, pairs, out_finish, 0)


def per_device(dims, unit, wide, q_slab, triangle, panel_q):
    nd, ny, nc, nx, nzl = dims
    nz, nr, nb = nd * nzl, ny * nc, nd * ny * nc
    rows, qk = q_slab.shape
    k_full, half = triangle.shape
    out_cols, narrow = panel_q.shape
    blocks = out_cols // (2 * unit)
    pairs = (blocks - 4 * wide) // 2 + wide
    chunks = 2 * pairs
    dma = pltpu.SemaphoreType.DMA
    far = pl.BlockSpec(memory_space=pl.ANY)
    return pl.pallas_call(
        functools.partial(kernel, dims, unit, (wide, pairs)),
        out_shape=jax.ShapeDtypeStruct((rows, out_cols), F32),
        in_specs=[pl.BlockSpec(memory_space=pltpu.VMEM), far, far],
        out_specs=far,
        scratch_shapes=[
            pltpu.VMEM((rows, qk), F32),
            pltpu.VMEM((k_full, half), F32),
            pltpu.VMEM((narrow, out_cols), F32),
            pltpu.VMEM((nb, rows // nr, qk), F32),
            pltpu.VMEM((rows // nr, k_full), F32),
            pltpu.VMEM((nd, nx, nr, rows // nr, half), F32),
            pltpu.VMEM((nx, rows, k_full), BF16),
            pltpu.VMEM((nx, rows, k_full), BF16),
            pltpu.VMEM((chunks, nd, nx, nzl, narrow, unit), F32),
            pltpu.VMEM((4, k_full, 2 * unit), BF16),
            pltpu.VMEM((4, k_full, 2 * unit), BF16),
            pltpu.VMEM((blocks, rows, 2 * unit), F32),
            dma((2,)),
            dma((nb,)), dma((nb,)),
            dma((chunks, nx)), dma((chunks, nx)), dma((chunks,)),
            dma((chunks, nz)), dma((chunks, nz)),
            dma((1,)), dma((1,)),
            dma((nx, 2)), dma((nx, 2)),
            dma((nx, 2, ny)), dma((nx, 2, ny)),
            dma((nx, 2, ny)), dma((nx, 2, ny)),
            dma((pairs,)), dma((blocks,)), dma((blocks,)),
        ],
        compiler_params=pltpu.CompilerParams(
            collective_id=0, has_side_effects=True, vmem_limit_bytes=57 * 1024 * 1024
        ),
    )(q_slab.T, triangle, panel_q.T)


def build(mesh, dims, unit, wide=1):
    torus = Mesh(mesh.devices.reshape(dims), AXES)
    slab = ("x", "zl")
    row = ("y", "core")
    in_specs = (P(slab, ("depth",) + row), P(None, "depth"), P(row, ("depth",) + slab))
    return jax.shard_map(
        functools.partial(per_device, dims, unit, wide),
        mesh=torus, in_specs=in_specs, out_specs=P(slab, row), check_vma=False)


def solution(mesh):
    return build(mesh, (mesh.shape["depth"], 4, 2, 4, 4), 128)
```

```python
import functools

import jax
import jax.numpy as jnp
from jax import lax
from jax.experimental import pallas as pl
from jax.experimental.pallas import tpu as pltpu
from jax.sharding import Mesh
from jax.sharding import PartitionSpec as P

AXES = ("depth", "y", "core", "x", "zl")
MESH = pl.DeviceIdType.MESH
F32, BF16 = jnp.float32, jnp.bfloat16


def split(value):
    high = value.astype(BF16)
    return high, (value - high.astype(F32)).astype(BF16)


def dot(a, b):
    return jnp.dot(a, b, preferred_element_type=F32)


def kernel(dims, unit, plan, q_ref, t_hbm, p_hbm, out_ref,
           qs, t_ref, p_ref, qbuf, qrow, lf, lhi, llo, gat, phi, plo, obuf, in_sem,
           q_send, q_recv, e_send, e_recv, e_own, z_send, z_recv,
           d_send, d_recv, lx_send, lx_recv, y_send, y_recv,
           c_send, c_recv, o_own, o_send, o_recv):
    wide, pairs = plan
    nd, ny, nc, nx, nzl = dims
    nz = nd * nzl
    nr = ny * nc
    nb = nd * nr
    d, y, core, x, zl = (lax.axis_index(a) for a in AXES)
    z = d * nzl + zl
    rk = y * nc + core
    me_b = d * nr + rk
    chunks = 2 * pairs
    ahead = 8
    piece = lf.shape[3]
    half = lf.shape[4]
    k_full = nd * half
    rows = nr * piece
    qk = qs.shape[1]

    def dev(**over):
        return tuple(over.get(a, v) for a, v in zip(AXES, (d, y, core, x, zl)))

    def at_z(pos):
        pos = lax.rem(pos + nz, nz)
        return lax.div(pos, nzl), lax.rem(pos, nzl)

    def at_b(pos):
        pos = lax.rem(pos, nb)
        dd, r = lax.div(pos, nr), lax.rem(pos, nr)
        return dd, lax.div(r, nc), lax.rem(r, nc), r

    def remote(src, dst, send, recv, to):
        return pltpu.make_async_remote_copy(
            src_ref=src, dst_ref=dst, send_sem=send, recv_sem=recv,
            device_id=to, device_id_type=MESH)

    def wide_before(m):
        return jnp.clip(m - 2, 0, wide)

    def base(m):
        return 2 * m + 2 * wide_before(m)

    def is_wide(m):
        return (m >= 2) & (m < 2 + wide)

    def role(pos, m):
        return lax.rem(pos + m + wide_before(m), 2)

    def share(pos, m):
        return jnp.where(is_wide(m), pos, role(pos, m))

    def partner_of(m):
        return lax.rem(x + 1 - 2 * role(x, m) + nx, nx)

    def receivers(m):
        return jnp.where(is_wide(m), nx - 1, 1)

    def receiver(m, s):
        return jnp.where(is_wide(m), lax.rem(x + s, nx), partner_of(m))

    def sender(m, s):
        return jnp.where(is_wide(m), lax.rem(x + nx - s, nx), partner_of(m))

    t_load = pltpu.make_async_copy(t_hbm, t_ref, in_sem.at[0])
    p_load = pltpu.make_async_copy(p_hbm, p_ref, in_sem.at[1])
    p_load.start()
    t_load.start()

    barrier = pltpu.get_barrier_semaphore()

    def greet(o, _):
        dd, yy, cc, _ = at_b(me_b + o)
        pl.semaphore_signal(barrier, inc=1, device_id=dev(depth=dd, y=yy, core=cc), device_id_type=MESH)
        return 0

    lax.fori_loop(1, nb, greet, 0)
    for o in range(1, nx):
        pl.semaphore_signal(barrier, inc=1, device_id=dev(x=lax.rem(x + o, nx)), device_id_type=MESH)
    for o in (1, nz - 1):
        dd, zz = at_z(z + o)
        pl.semaphore_signal(barrier, inc=1, device_id=dev(depth=dd, zl=zz), device_id_type=MESH)
    qs[...] = q_ref[...].T
    qbuf[me_b] = qs[pl.ds(pl.multiple_of(rk * piece, 8), piece), :]
    p_load.wait()
    pl.semaphore_wait(barrier, nb - 1 + nx - 1 + 2)

    def q_copy(o):
        dd, yy, cc, r = at_b(me_b + o)
        src = qs.at[pl.ds(pl.multiple_of(r * piece, 8), piece)]
        return remote(src, qbuf.at[me_b], q_send.at[o], q_recv.at[o], dev(depth=dd, y=yy, core=cc))

    def q_arrival(o):
        src = lax.rem(me_b + nb - o, nb)
        dd, yy, cc, _ = at_b(src)
        return remote(qbuf.at[src], qbuf.at[src], q_send.at[o], q_recv.at[o], dev(depth=dd, y=yy, core=cc))

    def e_rows(j, pos):
        m = lax.div(j, 2)
        start = (2 * (base(m) + share(pos, m)) + lax.rem(j, 2)) * unit
        return p_ref.at[:, pl.ds(pl.multiple_of(start, unit), unit)]

    def e_copy(j, o):
        to = lax.rem(x + o, nx)
        return remote(e_rows(j, to), gat.at[j, d, x, zl], e_send.at[j, o], e_recv.at[j, o], dev(x=to))

    def e_arrival(j, o):
        src = lax.rem(x + nx - o, nx)
        ref = gat.at[j, d, src, zl]
        return remote(ref, ref, e_send.at[j, o], e_recv.at[j, o], dev(x=src))

    def e_local(j):
        return pltpu.make_async_copy(e_rows(j, x), gat.at[j, d, x, zl], e_own.at[j])

    def e_start(j):
        for o in (1, nx - 1, 2):
            e_copy(j, o).start()
        e_local(j).start()

    def e_step(j, _):
        e_start(j)
        return 0

    def q_step(o, _):
        q_copy(o).start()
        return 0

    e_start(0)
    lax.fori_loop(1, nb, q_step, 0)
    lax.fori_loop(1, min(ahead, chunks), e_step, 0)

    nlong, nshort = nz // 2, (nz - 1) // 2

    def z_parts(j, hop, far, arriving):
        sign = 1 - 2 * lax.rem(j, 2)
        step = sign if far else -sign
        index = hop - 1 if far else nlong + hop - 1
        dd, zz = at_z(z - step * (hop if arriving else hop - 1))
        to_d, to_z = at_z(z - step if arriving else z + step)
        ref = gat.at[j, dd, :, zz]
        return remote(ref, ref, z_send.at[j, index], z_recv.at[j, index], dev(depth=to_d, zl=to_z))

    def z_copy(j, hop, far):
        return z_parts(j, hop, far, False)

    def z_arrival(j, hop, far):
        return z_parts(j, hop, far, True)

    def hop(j, h):
        if h == 1:
            e_local(j).wait()
            for o in (1, nx - 1, 2):
                e_arrival(j, o).wait_recv()
        for far, count in ((True, nlong), (False, nshort)):
            if 2 <= h <= count + 1:
                z_arrival(j, h - 1, far).wait_recv()
            if h <= count:
                z_copy(j, h, far).start()

    def step(g, h):
        for j in range(max(4 * g - 2, 0), 4 * g + 2):
            hop(j, h)

    ylong, yshort = ny // 2, (ny - 1) // 2
    ways = [(h, True) for h in range(1, ylong + 1)] + [(h, False) for h in range(1, yshort + 1)]

    def columns_of(e):
        return d if e == 0 else 1 - d

    def left_piece():
        def q_wait(o, _):
            q_arrival(o).wait_recv()
            return 0

        lax.fori_loop(1, nb, q_wait, 0)
        for b in range(nb):
            qrow[:, b * qk:(b + 1) * qk] = qbuf[b]
        t_load.wait()
        qh, ql = split(qrow[...])
        th, tl = split(t_ref[...])
        lf[d, x, rk] = dot(qh, th) + dot(qh, tl) + dot(ql, th)

    def depth_copy(e):
        ref = lf.at[columns_of(e), x, rk]
        return remote(ref, ref, d_send.at[0], d_recv.at[0], dev(depth=1 - d))

    def lx_copy(o, e):
        ref = lf.at[columns_of(e), x, rk]
        return remote(ref, ref, lx_send.at[o, e], lx_recv.at[o, e], dev(x=lax.rem(x + o, nx)))

    def lx_arrival(o, e):
        src = lax.rem(x + nx - o, nx)
        ref = lf.at[columns_of(e), src, rk]
        return remote(ref, ref, lx_send.at[o, e], lx_recv.at[o, e], dev(x=src))

    def y_index(h, far):
        return h - 1 if far else ylong + h - 1

    def y_step(xs, far):
        sign = 1 - 2 * lax.rem(xs, 2)
        return sign if far else -sign

    def y_parts(xs, e, h, far, arriving):
        step = y_step(xs, far)
        owner = lax.rem(y - step * (h if arriving else h - 1) + ny, ny)
        to = lax.rem((y - step if arriving else y + step) + ny, ny)
        ref = lf.at[columns_of(e), xs, owner * nc + core]
        i = y_index(h, far)
        return remote(ref, ref, y_send.at[xs, e, i], y_recv.at[xs, e, i], dev(y=to))

    def c_copy(xs, e, h, far, arriving=False):
        owner = lax.rem(y - y_step(xs, far) * h + ny, ny)
        i = 0 if h == 0 else 1 + y_index(h, far)
        ref = lf.at[columns_of(e), xs, owner * nc + (1 - core if arriving else core)]
        return remote(ref, ref, c_send.at[xs, e, i], c_recv.at[xs, e, i], dev(core=1 - core))

    def y_first(xs, e):
        for h, far in ways:
            if h == 1:
                y_parts(xs, e, 1, far, False).start()
        c_copy(xs, e, 0, True).start()

    def y_later(xs, e, h):
        for far, count in ((True, ylong), (False, yshort)):
            if 1 <= h - 1 <= count:
                y_parts(xs, e, h - 1, far, True).wait_recv()
                if h <= count:
                    y_parts(xs, e, h, far, False).start()
                c_copy(xs, e, h - 1, far).start()

    def left_ready(xs):
        for h, far in [(0, True)] + ways:
            for e in range(2):
                c_copy(xs, e, h, far, arriving=True).wait_recv()
        for b in range(nd):
            high, low = split(lf[b, xs].reshape(rows, half))
            lhi[xs, :, b * half:(b + 1) * half] = high
            llo[xs, :, b * half:(b + 1) * half] = low

    def piece_event():
        left_piece()
        depth_copy(0).start()
        for o in (1, nx - 1, 2):
            lx_copy(o, 0).start()
        y_first(x, 0)

    def lx_event(o, e):
        lx_arrival(o, e).wait_recv()
        y_first(lax.rem(x + nx - o, nx), e)

    def depth_event():
        depth_copy(1).wait_recv()
        for o in (1, nx - 1, 2):
            lx_copy(o, 1).start()

    near = (lax.rem(x + nx - 1, nx), lax.rem(x + 1, nx))
    across = lax.rem(x + 2, nx)

    def own_copy(m):
        start = (base(m) + share(x, m)) * 2 * unit
        dst = out_ref.at[:, pl.ds(pl.multiple_of(start, 2 * unit), 2 * unit)]
        return pltpu.make_async_copy(obuf.at[base(m)], dst, o_own.at[m])

    def ship(m, s, to, arriving=False):
        start = (base(m) + share(to if arriving else x, m)) * 2 * unit
        dst = out_ref.at[:, pl.ds(pl.multiple_of(start, 2 * unit), 2 * unit)]
        i = base(m) + s
        return remote(obuf.at[i], dst, o_send.at[i], o_recv.at[i], dev(x=to))

    def prepare(m):
        for part in range(2):
            high, low = split(gat[2 * m + part].reshape(k_full, unit))
            phi[lax.rem(m, 4), :, part * unit:(part + 1) * unit] = high
            plo[lax.rem(m, 4), :, part * unit:(part + 1) * unit] = low

    def product(m, i, xs):
        high, low = phi[lax.rem(m, 4)], plo[lax.rem(m, 4)]
        obuf[base(m) + i] = (dot(lhi[xs], high) + dot(lhi[xs], low)) + dot(llo[xs], high)

    def compute_others(m):
        prepare(m)

        def one(s, _):
            to = receiver(m, s)
            product(m, s, to)
            ship(m, s, to).start()
            return 0

        lax.fori_loop(1, receivers(m) + 1, one, 0)

    def compute_own(m):
        product(m, 0, x)
        own_copy(m).start()

    step(0, 1)
    step(1, 1)
    piece_event()
    step(0, 2)
    for o in (1, nx - 1):
        lx_event(o, 0)
    step(1, 2)
    depth_event()
    lax.fori_loop(ahead, chunks, e_step, 0)
    for xs in near:
        y_later(xs, 0, 2)
    step(0, 3)
    for o in (1, nx - 1):
        lx_event(o, 1)
    step(1, 3)
    for xs in near:
        y_later(xs, 1, 2)
    y_first(x, 1)
    y_later(x, 0, 2)
    for e in range(2):
        lx_event(2, e)
    step(0, 4)
    step(2, 1)
    for xs in near:
        for e in range(2):
            y_later(xs, e, 3)
    for xs in near:
        left_ready(xs)
    step(1, 4)
    step(0, 5)
    compute_others(0)
    y_later(x, 1, 2)
    for e in range(2):
        y_later(across, e, 2)
    step(2, 2)
    step(1, 5)
    compute_others(1)
    for e in range(2):
        y_later(x, e, 3)
        y_later(across, e, 3)
    step(2, 3)
    step(3, 1)
    left_ready(across)
    compute_others(2)
    step(2, 4)
    step(3, 2)
    left_ready(x)
    compute_own(0)
    compute_own(1)
    step(2, 5)
    compute_others(3)
    step(3, 3)
    compute_others(4)
    compute_own(2)
    step(3, 4)
    for m in range(5, pairs):
        hop(2 * m, 5)
        hop(2 * m + 1, 5)
        compute_others(m)
    for m in range(3, pairs):
        compute_own(m)

    def finish(j, _):
        for o in range(1, nx):
            e_copy(j, o).wait_send()
        for h in range(1, nlong + 1):
            z_copy(j, h, True).wait_send()
        for h in range(1, nshort + 1):
            z_copy(j, h, False).wait_send()
        return 0

    lax.fori_loop(0, chunks, finish, 0)

    def q_finish(o, _):
        q_copy(o).wait_send()
        return 0

    lax.fori_loop(1, nb, q_finish, 0)
    depth_copy(0).wait_send()
    for e in range(2):
        for o in range(1, nx):
            lx_copy(o, e).wait_send()

    def y_finish(xs, _):
        for e in range(2):
            c_copy(xs, e, 0, True).wait_send()
            for h, far in ways:
                c_copy(xs, e, h, far).wait_send()
                y_parts(xs, e, h, far, False).wait_send()
        return 0

    lax.fori_loop(0, nx, y_finish, 0)

    def out_finish(m, _):
        own_copy(m).wait()

        def one(s, _):
            ship(m, s, receiver(m, s)).wait_send()
            ship(m, s, sender(m, s), arriving=True).wait_recv()
            return 0

        lax.fori_loop(1, receivers(m) + 1, one, 0)
        return 0

    lax.fori_loop(0, pairs, out_finish, 0)


def per_device(dims, unit, wide, q_slab, triangle, panel_q):
    nd, ny, nc, nx, nzl = dims
    nz, nr, nb = nd * nzl, ny * nc, nd * ny * nc
    rows, qk = q_slab.shape
    k_full, half = triangle.shape
    out_cols, narrow = panel_q.shape
    blocks = out_cols // (2 * unit)
    pairs = (blocks - 4 * wide) // 2 + wide
    chunks = 2 * pairs
    dma = pltpu.SemaphoreType.DMA
    far = pl.BlockSpec(memory_space=pl.ANY)
    return pl.pallas_call(
        functools.partial(kernel, dims, unit, (wide, pairs)),
        out_shape=jax.ShapeDtypeStruct((rows, out_cols), F32),
        in_specs=[pl.BlockSpec(memory_space=pltpu.VMEM), far, far],
        out_specs=far,
        scratch_shapes=[
            pltpu.VMEM((rows, qk), F32),
            pltpu.VMEM((k_full, half), F32),
            pltpu.VMEM((narrow, out_cols), F32),
            pltpu.VMEM((nb, rows // nr, qk), F32),
            pltpu.VMEM((rows // nr, k_full), F32),
            pltpu.VMEM((nd, nx, nr, rows // nr, half), F32),
            pltpu.VMEM((nx, rows, k_full), BF16),
            pltpu.VMEM((nx, rows, k_full), BF16),
            pltpu.VMEM((chunks, nd, nx, nzl, narrow, unit), F32),
            pltpu.VMEM((4, k_full, 2 * unit), BF16),
            pltpu.VMEM((4, k_full, 2 * unit), BF16),
            pltpu.VMEM((blocks, rows, 2 * unit), F32),
            dma((2,)),
            dma((nb,)), dma((nb,)),
            dma((chunks, nx)), dma((chunks, nx)), dma((chunks,)),
            dma((chunks, nz)), dma((chunks, nz)),
            dma((1,)), dma((1,)),
            dma((nx, 2)), dma((nx, 2)),
            dma((nx, 2, ny)), dma((nx, 2, ny)),
            dma((nx, 2, ny)), dma((nx, 2, ny)),
            dma((pairs,)), dma((blocks,)), dma((blocks,)),
        ],
        compiler_params=pltpu.CompilerParams(
            collective_id=0, has_side_effects=True, vmem_limit_bytes=57 * 1024 * 1024
        ),
    )(q_slab.T, triangle, panel_q.T)


def build(mesh, dims, unit, wide=1):
    torus = Mesh(mesh.devices.reshape(dims), AXES)
    slab = ("x", "zl")
    row = ("y", "core")
    in_specs = (P(slab, ("depth",) + row), P(None, "depth"), P(row, ("depth",) + slab))
    return jax.shard_map(
        functools.partial(per_device, dims, unit, wide),
        mesh=torus, in_specs=in_specs, out_specs=P(slab, row), check_vma=False)


def solution(mesh):
    return build(mesh, (mesh.shape["depth"], 4, 2, 4, 4), 128)
```
